32 devices in a mesh: sp: 4 (over x, core), tp: 8 (over z, y).
Axes of the slice: x: 2, y: 2, z: 4, core: 2. Of those that a mesh axis runs over, the one named last changes fastest.
Arguments:
- tokens: bfloat16 [8, 220, 4096], P(None, 'sp'), may hold values from -6 to 6
- modulation: float32 [6, 4096], replicated, may hold values from -2.5 to 2.5
- w_qkv: bfloat16 [4096, 3, 4096], P('sp', None, 'tp'), may hold values from -4 to 4
- w_out: bfloat16 [4096, 4096], P('tp', 'sp'), may hold values from -0.09375 to 0.09375
- w_up: bfloat16 [4096, 16384], P('sp', 'tp'), may hold values from -0.09375 to 0.09375
- w_down: bfloat16 [16384, 4096], P('tp', 'sp'), may hold values from -0.046875 to 0.046875
Outputs:
- block_out: bfloat16 [8, 220, 4096], P(None, 'sp', 'tp')
The draws below stay inside these ranges and needn't reach their ends.
All inputs are finite; a program needn't handle non-finite values.
Results may differ from the reference program's by a relative error of at most 0.012.
Values may be sent and summed in bfloat16 or wider, within the bound.
No kernel may reach another device: no remote copies, remote signals or barrier semaphores. Data moves between devices by JAX's collectives and lax.ppermute only.
A program may use at most 128 MiB of HBM per device.

```python
import jax
import jax.numpy as jnp
from jax import lax

D = 4096
HEADS = 32
DH = 128
FF = 16384
FRAMES = 8
PATCHES = 220
N_TP = 8


def draw_w_qkv(key, part):
    inner = HEADS * DH
    base = jax.random.normal(key, (D, 3, inner), jnp.float32) * D ** (-0.5)
    factor = jnp.array([1.3, 1.3, 1.0], jnp.float32)
    base = base * factor[None, :, None]
    base = jnp.clip(base, -4.0, 4.0)
    return base.astype(jnp.bfloat16)


def block_scale(rng, shape, pieces, low, top_value):
    loudness = 1.0
    for axis_at, shards_of in pieces:
        steps = jax.random.uniform(jax.random.fold_in(jax.random.fold_in(rng, 6), axis_at), (shards_of,), jnp.float32, low / len(pieces), top_value / len(pieces))
        loudness = loudness * jnp.repeat(jnp.exp(steps), shape[axis_at] // shards_of).reshape((-1,) + (1,) * (len(shape) - 1 - axis_at))
    return loudness


def normal_values(stream_key, extent, scale, bound, cuts=(), held_as=jnp.bfloat16):
    level = block_scale(stream_key, extent, cuts, -0.22, 0.18) if cuts else 1.0
    drawn = jax.random.normal(stream_key, extent, jnp.float32) * scale * level
    return jnp.minimum(jnp.maximum(drawn, -bound), bound).astype(held_as)


def setup_inputs(seed: int = 0) -> dict:
    keys = jax.random.split(jax.random.key(seed), 7)
    tokens = normal_values(keys[0], (FRAMES, PATCHES, D), 1.0, 6.0, ((1, 4),))
    modulation = normal_values(keys[1], (6, D), 0.5, 2.5, (), jnp.float32)
    w_qkv = draw_w_qkv(jax.random.fold_in(keys[6], 71), 0)
    w_out = normal_values(keys[3], (HEADS * DH, D), (HEADS * DH) ** -0.5, 0.09375, ((0, 8), (1, 4)))
    w_up = normal_values(keys[4], (D, FF), D ** -0.5, 0.09375, ((0, 4), (1, 8)))
    w_down = normal_values(keys[5], (FF, D), FF ** -0.5, 0.046875, ((0, 8), (1, 4)))
    return {"tokens": tokens, "modulation": modulation, "w_qkv": w_qkv, "w_out": w_out, "w_up": w_up, "w_down": w_down}


EPSILON = 1e-06

def normalize(tok_rows, shift_vec, scale_vec):
    values = tok_rows.astype(jnp.float32)
    center = lax.optimization_barrier(jnp.mean(values, axis=-1, keepdims=True))
    spread = lax.optimization_barrier(jnp.mean(jnp.square(values - center), axis=-1, keepdims=True))
    scaled = (values - center) * lax.rsqrt(spread + EPSILON)
    return (scaled * (1.0 + scale_vec) + shift_vec).astype(jnp.bfloat16)

def attend_single(triple):
    query_rows, key_rows, value_rows = triple
    factor = query_rows.shape[-1] ** (-0.5)
    scores = lax.dot_general(query_rows, key_rows, (((1,), (1,)), ((), ())), preferred_element_type=jnp.float32) * factor
    row_max = lax.optimization_barrier(jnp.max(scores, axis=1, keepdims=True))
    raw_weights = jnp.exp(scores - row_max)
    att_weights = (raw_weights / lax.optimization_barrier(jnp.sum(raw_weights, axis=1, keepdims=True))).astype(jnp.bfloat16)
    return jnp.dot(att_weights, value_rows, preferred_element_type=jnp.float32).astype(jnp.bfloat16)

def reference(tokens, modulation, w_qkv, w_out, w_up, w_down):
    frames, patches, width = tokens.shape
    heads_local = HEADS // N_TP
    inner = heads_local * DH
    hidden_local = FF // N_TP
    mod_a = normalize(tokens, modulation[0], modulation[1]).reshape(frames * patches, width)

    def attn_group(group, running):
        begin = (group * inner).astype(jnp.int32)
        weight_group = lax.dynamic_slice_in_dim(w_qkv, begin, inner, 2).reshape(width, 3 * inner)
        projected = jnp.dot(mod_a, weight_group, preferred_element_type=jnp.float32).astype(jnp.bfloat16)
        projected = projected.reshape(frames, patches, 3, heads_local, DH)
        stacked = jnp.transpose(projected, (2, 0, 3, 1, 4)).reshape(3, frames * heads_local, patches, DH)
        attended = lax.map(attend_single, (stacked[0], stacked[1], stacked[2]))
        attended = attended.reshape(frames, heads_local, patches, DH)
        rows_group = lax.dynamic_slice_in_dim(w_out, begin, inner, 0).reshape(heads_local, DH, width)
        term = jnp.einsum('fhpd,hde->fpe', attended.astype(jnp.float32), rows_group.astype(jnp.float32))
        term = lax.optimization_barrier(term.astype(jnp.bfloat16)).astype(jnp.float32)
        return running + term
    attn_sum = lax.fori_loop(0, N_TP, attn_group, jnp.zeros((frames, patches, width), jnp.float32))
    middle = (tokens.astype(jnp.float32) + modulation[2] * attn_sum).astype(jnp.bfloat16)
    mod_b = normalize(middle, modulation[3], modulation[4]).reshape(frames * patches, width)

    def mlp_group(group, running):
        begin = (group * hidden_local).astype(jnp.int32)
        up_cols = lax.dynamic_slice_in_dim(w_up, begin, hidden_local, 1)
        hidden = jax.nn.gelu(jnp.dot(mod_b, up_cols, preferred_element_type=jnp.float32), approximate=True).astype(jnp.bfloat16)
        down_rows = lax.dynamic_slice_in_dim(w_down, begin, hidden_local, 0)
        term = jnp.dot(hidden, down_rows, preferred_element_type=jnp.float32)
        term = lax.optimization_barrier(term.astype(jnp.bfloat16)).astype(jnp.float32)
        return running + term.reshape(frames, patches, width)
    mlp_sum = lax.fori_loop(0, N_TP, mlp_group, jnp.zeros((frames, patches, width), jnp.float32))
    return (middle.astype(jnp.float32) + modulation[5] * mlp_sum).astype(jnp.bfloat16)
```

```python
import functools

import jax
import jax.numpy as jnp
from jax import lax
from jax.experimental import pallas as pl
from jax.experimental.pallas import tpu as pltpu
from jax.sharding import PartitionSpec as P

DH = 128
EPSILON = 1e-06
BF16 = jnp.bfloat16
F32 = jnp.float32
VMEM_LIMIT = 60 * 1024 * 1024


def normalize(tok_rows, shift_vec, scale_vec):
    values = tok_rows.astype(F32)
    center = jnp.mean(values, axis=-1, keepdims=True)
    spread = jnp.mean(jnp.square(values - center), axis=-1, keepdims=True)
    scaled = (values - center) * lax.rsqrt(spread + EPSILON)
    return (scaled * (1.0 + scale_vec) + shift_vec).astype(BF16)


def project_rows(operand, weight, einsum_form):
    return jnp.einsum(
        einsum_form,
        operand,
        lax.all_gather(weight, "sp", axis=0, tiled=True),
        preferred_element_type=F32,
    )


def project_cols(operand, weight, einsum_form, leading):
    portion = lax.all_gather(weight, "sp", axis=1, tiled=True)
    shaped = portion.reshape(leading + (portion.shape[1],))
    return jnp.einsum(einsum_form, operand, shaped, preferred_element_type=F32)


def attend_items(pieces):
    queries, key_rows, values = pieces
    factor = queries.shape[-1] ** (-0.5)

    def single(triple):
        query_one, key_one, value_one = triple
        scores = (
            lax.dot_general(
                query_one, key_one, (((1,), (1,)), ((), ())), preferred_element_type=F32
            )
            * factor
        )
        row_max = jnp.max(scores, axis=1, keepdims=True)
        raw_weights = jnp.exp(scores - row_max)
        att_weights = (raw_weights / jnp.sum(raw_weights, axis=1, keepdims=True)).astype(BF16)
        return jnp.dot(att_weights, value_one, preferred_element_type=F32).astype(BF16)

    result = lax.map(single, (queries[0], key_rows[0], values[0]))
    return result[None]


def general_shards(tokens, modulation, w_qkv, w_out, w_up, w_down):
    frames, patches, width = tokens.shape
    heads_local = w_qkv.shape[2] // DH
    sp_count = lax.axis_size("sp")
    tp_count = lax.axis_size("tp")
    items_dev = heads_local * frames // sp_count
    mod_a = normalize(tokens, modulation[0], modulation[1])
    weight_qkv = w_qkv.reshape(w_qkv.shape[0], 3, heads_local, DH)
    projected = project_rows(mod_a, weight_qkv, "fpd,dshe->shfpe").astype(BF16)
    projected = projected.reshape(3, sp_count, items_dev, patches, DH)
    attended = attend_items(
        tuple(
            lax.all_to_all(projected[i], "sp", split_axis=0, concat_axis=2, tiled=True)
            for i in range(3)
        )
    )
    returned = lax.all_to_all(attended, "sp", split_axis=2, concat_axis=0, tiled=True)
    returned = returned.reshape(heads_local, frames, patches, DH)
    partial_attn = project_cols(returned, w_out, "hfpd,hde->fpe", (heads_local, DH))
    summed = lax.psum(partial_attn.astype(BF16), "tp").astype(F32)
    middle = (tokens.astype(F32) + modulation[2] * summed).astype(BF16)
    mod_b = normalize(middle, modulation[3], modulation[4])
    up_proj = project_rows(mod_b, w_up, "fpd,dc->fpc")
    hidden = jax.nn.gelu(up_proj, approximate=True).astype(BF16)
    partial_mlp = project_cols(hidden, w_down, "fpk,kc->fpc", (w_down.shape[0],))
    part = width // tp_count
    offset = lax.axis_index("tp") * part
    base_mine = lax.dynamic_slice_in_dim(middle, offset, part, 2).astype(F32)
    gate_mine = lax.dynamic_slice_in_dim(modulation[5], offset, part, 0)
    share = lax.psum_scatter(
        partial_mlp.astype(BF16), "tp", scatter_dimension=2, tiled=True
    ).astype(F32)
    return (base_mine + gate_mine * share).astype(BF16)


def row_block(rows):
    for parts in (5, 4, 3, 2, 7):
        if rows % (8 * parts) == 0:
            return rows // parts
    return rows


def ln_kernel(count, idx_ref, shift_ref, scale_ref, *refs):
    pieces, out_ref = refs[:count], refs[count]
    width = sum(p.shape[1] for p in pieces)
    vals = [p[...].astype(F32) for p in pieces]
    center = sum(jnp.sum(v, axis=1, keepdims=True) for v in vals) / width
    devs = [v - center for v in vals]
    spread = sum(jnp.sum(d * d, axis=1, keepdims=True) for d in devs) / width
    inv = lax.rsqrt(spread + EPSILON)
    for i, d in enumerate(devs):
        cw = d.shape[1]
        cols = pl.ds(pl.multiple_of(idx_ref[i] * cw, cw), cw)
        gain = 1.0 + scale_ref[:, cols]
        out_ref[:, cols] = (d * inv * gain + shift_ref[:, cols]).astype(BF16)


def layer_norm(pieces, cols, shift_vec, scale_vec):
    rows = pieces[0].shape[0]
    width = sum(p.shape[1] for p in pieces)
    tile = row_block(rows)
    vec = pl.BlockSpec((1, width), lambda i, idx: (0, 0))
    return pl.pallas_call(
        functools.partial(ln_kernel, len(pieces)),
        grid_spec=pltpu.PrefetchScalarGridSpec(
            num_scalar_prefetch=1,
            grid=(rows // tile,),
            in_specs=[vec, vec]
            + [pl.BlockSpec((tile, p.shape[1]), lambda i, idx: (i, 0)) for p in pieces],
            out_specs=pl.BlockSpec((tile, width), lambda i, idx: (i, 0)),
        ),
        out_shape=jax.ShapeDtypeStruct((rows, width), BF16),
        compiler_params=pltpu.CompilerParams(vmem_limit_bytes=VMEM_LIMIT),
        cost_estimate=pl.CostEstimate(
            flops=10 * rows * width, bytes_accessed=4 * rows * width, transcendentals=rows
        ),
        name="ln",
    )(cols, shift_vec[None], scale_vec[None], *pieces)


def gelu(v):
    return 0.5 * v * (1.0 + jnp.tanh(0.7978845608028654 * (v + 0.044715 * v * v * v)))


def k_shards_kernel(n, act, idx_ref, a_ref, *refs):
    ws, out_ref = refs[:n], refs[n]
    depth = ws[0].shape[0]
    acc = None
    for r in range(n):
        cols = pl.ds(pl.multiple_of(idx_ref[r] * depth, depth), depth)
        term = jnp.dot(a_ref[:, cols], ws[r][...], preferred_element_type=F32)
        acc = term if acc is None else acc + term
    out_ref[...] = (gelu(acc) if act else acc).astype(BF16)


def matmul_k_shards(a, shards_in, order, act, tile):
    n = len(shards_in)
    rows, depth_all = a.shape
    depth, cols = shards_in[0].shape
    return pl.pallas_call(
        functools.partial(k_shards_kernel, n, act),
        grid_spec=pltpu.PrefetchScalarGridSpec(
            num_scalar_prefetch=1,
            grid=(cols // tile,),
            in_specs=[pl.BlockSpec((rows, depth_all), lambda j, idx: (0, 0))]
            + [pl.BlockSpec((depth, tile), lambda j, idx: (0, j))] * n,
            out_specs=pl.BlockSpec((rows, tile), lambda j, idx: (0, j)),
        ),
        out_shape=jax.ShapeDtypeStruct((rows, cols), BF16),
        compiler_params=pltpu.CompilerParams(vmem_limit_bytes=VMEM_LIMIT),
        cost_estimate=pl.CostEstimate(
            flops=2 * rows * depth_all * cols,
            bytes_accessed=2 * (rows * depth_all + depth_all * cols + rows * cols),
            transcendentals=0,
        ),
        name="mm_k",
    )(order, a, *shards_in)


def n_shards_kernel(n, parts, idx_ref, *refs):
    a_parts, ws, out_ref, a_ref = refs[:parts], refs[parts : parts + n], refs[-2], refs[-1]
    step = pl.program_id(0)
    if parts > 1:

        @pl.when(step == 0)
        def _():
            for i in range(parts):
                cw = a_parts[i].shape[1]
                cols = pl.ds(pl.multiple_of(idx_ref[n + 1 + i] * cw, cw), cw)
                a_ref[:, cols] = a_parts[i][...]

    source = a_ref if parts > 1 else a_parts[0]
    for r in range(n):

        @pl.when(step == r)
        def _():
            out_ref[0] = jnp.dot(
                source[...], ws[r][...], preferred_element_type=F32
            ).astype(BF16)


def matmul_n_shards(a_parts, part_cols, shards_in, slots, half, chunk):
    n, parts = len(shards_in), len(a_parts)
    rows = a_parts[0].shape[0]
    depth = shards_in[0].shape[0]
    idx = jnp.concatenate([slots, half[None], part_cols]).astype(jnp.int32)
    full = lambda i, idx: (0, 0)
    return pl.pallas_call(
        functools.partial(n_shards_kernel, n, parts),
        grid_spec=pltpu.PrefetchScalarGridSpec(
            num_scalar_prefetch=1,
            grid=(n,),
            in_specs=[pl.BlockSpec(p.shape, full) for p in a_parts]
            + [pl.BlockSpec((depth, chunk), lambda i, idx: (0, idx[n]))] * n,
            out_specs=pl.BlockSpec((1, rows, chunk), lambda i, idx: (idx[i], 0, 0)),
            scratch_shapes=[pltpu.VMEM((rows, depth) if parts > 1 else (8, 128), BF16)],
        ),
        out_shape=jax.ShapeDtypeStruct((n, rows, chunk), BF16),
        compiler_params=pltpu.CompilerParams(vmem_limit_bytes=VMEM_LIMIT),
        cost_estimate=pl.CostEstimate(
            flops=2 * rows * depth * chunk * n,
            bytes_accessed=2 * (rows * depth + n * depth * chunk + n * rows * chunk),
            transcendentals=0,
        ),
        name="mm_n",
    )(idx, *a_parts, *shards_in)


def attention_kernel(n, frames, patches, *refs):
    ins, outs = refs[: 3 * n], refs[3 * n : 4 * n]
    wide, back = refs[4 * n], refs[4 * n + 1]
    rows = frames * patches
    padded = patches + (-patches) % 8
    factor = DH ** (-0.5)
    for j in range(3):
        for r in range(n):
            wide[j, r, :rows, :] = ins[j * n + r][...].astype(F32)
            wide[j, r, rows:, :] = jnp.zeros((frames * (padded - patches), DH), F32)
    keys_at = lax.broadcasted_iota(jnp.int32, (n * padded, n * padded), 1)
    keep = lax.rem(keys_at, padded) < patches

    def frame(f, carry):
        def rows_of(j):
            return jnp.concatenate(
                [wide[j, r, pl.ds(f, padded, stride=frames), :] for r in range(n)], axis=0
            ).astype(BF16)

        query, key, value = rows_of(0), rows_of(1), rows_of(2)
        scores = (
            lax.dot_general(query, key, (((1,), (1,)), ((), ())), preferred_element_type=F32)
            * factor
        )
        scores = jnp.where(keep, scores, -jnp.inf)
        raw = jnp.exp(scores - jnp.max(scores, axis=1, keepdims=True))
        weights = (raw / jnp.sum(raw, axis=1, keepdims=True)).astype(BF16)
        result = jnp.dot(weights, value, preferred_element_type=F32)
        for r in range(n):
            back[r, pl.ds(f, padded, stride=frames), :] = result[r * padded : (r + 1) * padded]
        return carry

    for f in range(frames):
        frame(f, 0)
    for r in range(n):
        outs[r][...] = back[r, :rows, :].astype(BF16)


def attention(pieces, n, frames, patches):
    rows = frames * patches
    padded = patches + (-patches) % 8
    block = jax.ShapeDtypeStruct((rows, DH), BF16)
    return pl.pallas_call(
        functools.partial(attention_kernel, n, frames, patches),
        in_specs=[pl.BlockSpec(memory_space=pltpu.VMEM)] * (3 * n),
        out_specs=[pl.BlockSpec(memory_space=pltpu.VMEM)] * n,
        out_shape=[block] * n,
        scratch_shapes=[
            pltpu.VMEM((3, n, frames * padded, DH), F32),
            pltpu.VMEM((n, frames * padded, DH), F32),
        ],
        compiler_params=pltpu.CompilerParams(vmem_limit_bytes=VMEM_LIMIT),
        cost_estimate=pl.CostEstimate(
            flops=4 * frames * (n * patches) ** 2 * DH,
            bytes_accessed=8 * n * rows * DH,
            transcendentals=frames * (n * patches) ** 2,
        ),
        name="attend",
    )(*[pieces[j][r] for j in range(3) for r in range(n)])


def swap(value, axis, bits):
    size = lax.axis_size(axis)
    return lax.ppermute(value, axis, [(i, i ^ bits) for i in range(size)])


def after(value, *earlier):
    return lax.optimization_barrier((value,) + earlier)[0]


def gather_sp(weight, n):
    got = {0: weight}
    for r in range(2, n, 2):
        got[r] = swap(weight, "sp", r)
    got[1] = swap(weight, "sp", 1)
    for r in range(3, n, 2):
        got[r] = swap(got[r - 1], "sp", 1)
    return [got[r] for r in range(n)]


def scatter_sum(other, mine, nz):
    total = {}
    for k in range(nz - 1, -1, -1):
        came = swap(other[k], "tp", 1)
        total[k] = mine[k].astype(F32) + came.astype(F32)
    result = total[0]
    for k in range(nz - 1, 0, -1):
        result = result + swap(total[k].astype(BF16), "tp", 2 * k).astype(F32)
    return result


def spread_tp(piece, nz):
    same = {0: piece}
    for k in range(nz - 1, 0, -1):
        same[k] = swap(piece, "tp", 2 * k)
    other = {0: swap(piece, "tp", 1)}
    for k in range(nz - 1, 0, -1):
        other[k] = swap(same[k], "tp", 1)
    return [same[k] for k in range(nz)], [other[k] for k in range(nz)]


def shards(tokens, modulation, w_qkv, w_out, w_up, w_down):
    frames, patches, width = tokens.shape
    n = lax.axis_size("sp")
    n_tp = lax.axis_size("tp")
    nz = n_tp // 2
    rows = frames * patches
    chunk = width // n_tp
    s, t = lax.axis_index("sp"), lax.axis_index("tp")
    y, z = t % 2, t // 2
    rel = s ^ jnp.arange(n, dtype=jnp.int32)
    slots = rel ^ z
    zrel = z ^ jnp.arange(nz, dtype=jnp.int32)

    flat = tokens.transpose(1, 0, 2).reshape(rows, width)
    weight_qkv = w_qkv.transpose(1, 0, 2)
    shards_qkv = [gather_sp(weight_qkv[j], n) for j in range(3)]
    shards_out = gather_sp(w_out, n)

    mod_a = layer_norm([flat], jnp.zeros((1,), jnp.int32), modulation[0], modulation[1])
    pieces = []
    sent = []
    for j in range(3):
        projected = matmul_k_shards(mod_a, shards_qkv[j], rel, False, w_qkv.shape[2])
        cut = [
            lax.dynamic_slice_in_dim(projected, (s ^ r) * DH, DH, 1) for r in range(n)
        ]
        pieces.append([cut[0]] + [swap(cut[r], "sp", r) for r in range(1, n)])
    attended = attention(pieces, n, frames, patches)
    returned = [attended[0]] + [swap(attended[r], "sp", r) for r in range(1, n)]

    shards_up = gather_sp(after(w_up, *attended), n)
    shards_down = gather_sp(after(w_down, *attended), n)

    terms_other = matmul_n_shards(returned, rel, shards_out, slots, 1 - y, chunk)
    terms_mine = matmul_n_shards(returned, rel, shards_out, slots, y, chunk)
    attn_sum = scatter_sum(terms_other, terms_mine, nz)
    offset = t * chunk
    own = lambda v: lax.dynamic_slice_in_dim(v, offset, chunk, v.ndim - 1)
    middle = (own(flat).astype(F32) + own(modulation[2]) * attn_sum).astype(BF16)
    same, other = spread_tp(middle, nz)
    mod_b = layer_norm(
        same + other,
        jnp.concatenate([zrel * 2 + y, zrel * 2 + 1 - y]),
        modulation[3],
        modulation[4],
    )
    hidden = matmul_k_shards(mod_b, shards_up, rel, True, w_up.shape[1] // 8)
    none = jnp.zeros((1,), jnp.int32)
    terms_other = matmul_n_shards([hidden], none, shards_down, slots, 1 - y, chunk)
    terms_mine = matmul_n_shards([hidden], none, shards_down, slots, y, chunk)
    mlp_sum = scatter_sum(terms_other, terms_mine, nz)
    block_out = (middle.astype(F32) + own(modulation[5]) * mlp_sum).astype(BF16)
    return block_out.reshape(patches, frames, chunk).transpose(1, 0, 2)


def power_of_two(v):
    return v & (v - 1) == 0


def solution(mesh):
    placed = (
        P(None, "sp", None),
        P(),
        P("sp", None, "tp"),
        P("tp", "sp"),
        P("sp", "tp"),
        P("tp", "sp"),
    )
    n, n_tp = mesh.shape["sp"], mesh.shape["tp"]

    def body(tokens, modulation, w_qkv, w_out, w_up, w_down):
        fits = (
            power_of_two(n)
            and n_tp == 2 * n
            and w_qkv.shape[2] == n * DH
            and tokens.shape[0] == 8
        )
        chosen = shards if fits else general_shards
        return chosen(tokens, modulation, w_qkv, w_out, w_up, w_down)

    return jax.shard_map(
        body, mesh=mesh, in_specs=placed, out_specs=P(None, "sp", "tp"), check_vma=False
    )
```
